32 devices in a mesh: pop: 16 (over z, x, core), hid: 2 (over y).
Axes of the slice: x: 2, y: 2, z: 4, core: 2. Of those that a mesh axis runs over, the one named last changes fastest.
Arguments:
- tokens: bfloat16 [512, 4096], P('pop', 'hid'), may hold values from -6 to 6
- fitness_ranks: int32 [32], replicated, may hold values from 0 to 31, each once
- gate_weight: bfloat16 [4096, 16384], P('hid', 'pop'), may hold values from -0.09375 to 0.09375
- up_weight: bfloat16 [4096, 16384], P('hid', 'pop'), may hold values from -0.09375 to 0.09375
- down_weight: bfloat16 [16384, 4096], P('pop', 'hid'), may hold values from -0.046875 to 0.046875
- gate_input_factor: bfloat16 [32, 4, 4096], P(None, None, 'hid'), may hold values from -6 to 6
- up_input_factor: bfloat16 [32, 4, 4096], P(None, None, 'hid'), may hold values from -6 to 6
- down_right: bfloat16 [32, 4, 4096], P(None, None, 'hid'), may hold values from -6 to 6
- gate_output_factor: bfloat16 [32, 4, 16384], P('pop'), may hold values from -6 to 6
- up_output_factor: bfloat16 [32, 4, 16384], P('pop'), may hold values from -6 to 6
- down_left: bfloat16 [32, 4, 16384], P('pop'), may hold values from -6 to 6
Outputs:
- mixed: bfloat16 [512, 4096], P('pop', 'hid')
- gate_step: float32 [4096, 16384], P('hid', 'pop')
- up_step: float32 [4096, 16384], P('hid', 'pop')
- down_step: float32 [16384, 4096], P('pop', 'hid')
The draws below stay inside these ranges and needn't reach their ends.
Inputs may be any that keep to these rules, and one draw needn't show every extreme that they name: `fitness_ranks`: every rank appears exactly once.
All inputs are finite; a program needn't handle non-finite values.
Results may differ from the reference program's by a relative error of at most 0.025.
Values may be sent and summed in bfloat16 or wider, within the bound.
No kernel may reach another device: no remote copies, remote signals or barrier semaphores. Data moves between devices by JAX's collectives and lax.ppermute only.
A program may use at most 128 MiB of HBM per device.

```python
import math
import jax
import jax.numpy as jnp
from jax import lax

MODEL_WIDTH = 4096
HIDDEN_UNITS = 16384
RANK = 4
SAMPLE_LENGTH = 16
CANDIDATE_NUMBER = 32
TOTAL_TOKENS = 512
N_POP = 16


def steps_of(rng, shape, split, low, high):
    def one(axis_at, shards_of):
        heights = jax.random.uniform(jax.random.fold_in(jax.random.fold_in(rng, 6), axis_at), (shards_of,), jnp.float32, low / len(split), high / len(split))
        return jnp.repeat(jnp.exp(heights), shape[axis_at] // shards_of).reshape((-1,) + (1,) * (len(shape) - axis_at - 1))

    gain = one(*split[0])
    for cut in split[1:]:
        gain = gain * one(*cut)
    return gain


def noise(own_key, extent, scale, reach, split=(), kind=jnp.bfloat16):
    factor_of = steps_of(own_key, extent, split, -0.22, 0.18) if split else 1.0
    array = jax.random.normal(own_key, extent, jnp.float32) * scale * factor_of
    return jnp.minimum(jnp.maximum(array, -reach), reach).astype(kind)


def setup_inputs(seed: int = 0) -> dict:
    streams_of = jax.random.split(jax.random.key(seed), 12)
    tokens = noise(streams_of[0], (TOTAL_TOKENS, MODEL_WIDTH), 1.0, 6.0, ((0, 16), (1, 2)))
    fitness_ranks = jax.random.permutation(streams_of[1], CANDIDATE_NUMBER).astype(jnp.int32)
    gate_weight = noise(streams_of[2], (MODEL_WIDTH, HIDDEN_UNITS), MODEL_WIDTH ** -0.5, 0.09375, ((0, 2), (1, 16)))
    up_weight = noise(streams_of[3], (MODEL_WIDTH, HIDDEN_UNITS), MODEL_WIDTH ** -0.5, 0.09375, ((0, 2), (1, 16)))
    down_weight = noise(streams_of[4], (HIDDEN_UNITS, MODEL_WIDTH), HIDDEN_UNITS ** -0.5, 0.046875, ((0, 16), (1, 2)))
    gate_input_factor = noise(streams_of[5], (CANDIDATE_NUMBER, RANK, MODEL_WIDTH), 1.0, 6.0, ((2, 2),))
    up_input_factor = noise(streams_of[6], (CANDIDATE_NUMBER, RANK, MODEL_WIDTH), 1.0, 6.0, ((2, 2),))
    down_right = noise(streams_of[7], (CANDIDATE_NUMBER, RANK, MODEL_WIDTH), 1.0, 6.0, ((2, 2),))
    gate_output_factor = noise(streams_of[8], (CANDIDATE_NUMBER, RANK, HIDDEN_UNITS), 1.0, 6.0, ((0, 16),))
    up_output_factor = noise(streams_of[9], (CANDIDATE_NUMBER, RANK, HIDDEN_UNITS), 1.0, 6.0, ((0, 16),))
    down_left = noise(streams_of[10], (CANDIDATE_NUMBER, RANK, HIDDEN_UNITS), 1.0, 6.0, ((0, 16),))
    return dict(tokens=tokens, fitness_ranks=fitness_ranks, gate_weight=gate_weight, up_weight=up_weight, down_weight=down_weight, gate_input_factor=gate_input_factor, up_input_factor=up_input_factor, down_right=down_right, gate_output_factor=gate_output_factor, up_output_factor=up_output_factor, down_left=down_left)


def reference(tokens, fitness_ranks, gate_weight, up_weight, down_weight, gate_input_factor, up_input_factor, down_right, gate_output_factor, up_output_factor, down_left):
    scalar_real = jnp.float32
    fitness = fitness_ranks.astype(scalar_real) / (CANDIDATE_NUMBER - 1) - 0.5
    scale_in = 0.5 / math.sqrt(MODEL_WIDTH * RANK)
    scale_out = 0.5 / math.sqrt(HIDDEN_UNITS * RANK)
    member_wise = tokens.reshape(CANDIDATE_NUMBER, SAMPLE_LENGTH, MODEL_WIDTH).astype(scalar_real)
    gate_projection = jnp.einsum('otl,ozl->otz', member_wise, gate_input_factor.astype(scalar_real))
    up_projection = jnp.einsum('otl,ozl->otz', member_wise, up_input_factor.astype(scalar_real))
    gate_lowrank_term = jnp.einsum('iln,ina->ila', gate_projection, gate_output_factor.astype(scalar_real)).reshape(TOTAL_TOKENS, HIDDEN_UNITS)
    gate = jnp.dot(tokens, gate_weight, preferred_element_type=scalar_real) + scale_in * gate_lowrank_term
    up_lowrank_term = jnp.einsum('iln,ina->ila', up_projection, up_output_factor.astype(scalar_real)).reshape(TOTAL_TOKENS, HIDDEN_UNITS)
    up = jnp.dot(tokens, up_weight, preferred_element_type=scalar_real) + scale_in * up_lowrank_term
    hidden = (jax.nn.silu(gate) * up).astype(jnp.bfloat16)
    embedding_dimension = HIDDEN_UNITS // N_POP
    output_factor_single = down_right.astype(scalar_real)

    def add_block(block, total):
        start = (block * embedding_dimension).astype(jnp.int32)
        zero = jnp.int32(0)
        inner_feature_slab = lax.dynamic_slice(hidden, (zero, start), (TOTAL_TOKENS, embedding_dimension))
        weight_block = lax.dynamic_slice(down_weight, (start, zero), (embedding_dimension, MODEL_WIDTH))
        left_matrix_slab = lax.dynamic_slice(down_left, (zero, zero, start), (CANDIDATE_NUMBER, RANK, embedding_dimension))
        contracting_matrix = jnp.einsum('reu,ryu->rey', inner_feature_slab.reshape(CANDIDATE_NUMBER, SAMPLE_LENGTH, embedding_dimension).astype(scalar_real), left_matrix_slab.astype(scalar_real))
        lowrank_product = jnp.einsum('okw,owt->okt', contracting_matrix, output_factor_single).reshape(TOTAL_TOKENS, MODEL_WIDTH)
        term = jnp.dot(inner_feature_slab, weight_block, preferred_element_type=scalar_real) + scale_out * lowrank_product
        rounded = lax.optimization_barrier(term.astype(jnp.bfloat16))
        return total + rounded.astype(scalar_real)
    summed = lax.fori_loop(0, N_POP, add_block, jnp.zeros((TOTAL_TOKENS, MODEL_WIDTH), scalar_real))
    mixed = summed.astype(jnp.bfloat16)
    factor = 1.0 / math.sqrt(CANDIDATE_NUMBER * RANK)
    weights3 = fitness[:, None, None]
    scaled_gate = (gate_input_factor.astype(scalar_real) * weights3).astype(jnp.bfloat16).reshape(CANDIDATE_NUMBER * RANK, MODEL_WIDTH)
    scaled_up = (up_input_factor.astype(scalar_real) * weights3).astype(jnp.bfloat16).reshape(CANDIDATE_NUMBER * RANK, MODEL_WIDTH)
    scaled_down = (down_right.astype(scalar_real) * weights3).astype(jnp.bfloat16).reshape(CANDIDATE_NUMBER * RANK, MODEL_WIDTH)
    dims = (((0,), (0,)), ((), ()))
    gate_step = factor * lax.dot_general(scaled_gate, gate_output_factor.reshape(CANDIDATE_NUMBER * RANK, HIDDEN_UNITS), dims, preferred_element_type=scalar_real)
    up_step = factor * lax.dot_general(scaled_up, up_output_factor.reshape(CANDIDATE_NUMBER * RANK, HIDDEN_UNITS), dims, preferred_element_type=scalar_real)
    down_step = factor * lax.dot_general(down_left.reshape(CANDIDATE_NUMBER * RANK, HIDDEN_UNITS), scaled_down, dims, preferred_element_type=scalar_real)
    return (mixed, gate_step, up_step, down_step)
```

```python
import functools
import math

import jax
import jax.numpy as jnp
from jax import lax
from jax.experimental import pallas as pl
from jax.experimental.pallas import tpu as pltpu
from jax.sharding import PartitionSpec as P

MODEL_WIDTH = 4096
HIDDEN_UNITS = 16384
RANK = 4
SAMPLE_LENGTH = 16
X_COUNT = 2
CORE_COUNT = 2
PLANE = X_COUNT * CORE_COUNT
LANES = 128
F32 = jnp.float32
BF16 = jnp.bfloat16


def dot(a, b):
    return jnp.dot(a, b, preferred_element_type=F32)


def dot_nt(a, b):
    return lax.dot_general(a, b, (((1,), (1,)), ((), ())), preferred_element_type=F32)


def split_high_low(v):
    high = v.astype(BF16)
    return high, (v - high.astype(F32)).astype(BF16)


def place():
    p = lax.axis_index("pop")
    y = lax.axis_index("hid")
    return p // PLANE, (p // CORE_COUNT) % X_COUNT, p % CORE_COUNT, y


def iota(shape, dim):
    return lax.broadcasted_iota(jnp.int32, shape, dim)


def row_members(shape, members):
    unit = iota(shape, 0) // SAMPLE_LENGTH
    out = jnp.zeros(shape, jnp.int32)
    for index, member in enumerate(members):
        out = jnp.where(unit == index, member, out)
    return out


def compiler_params(limit_mib):
    return pltpu.CompilerParams(vmem_limit_bytes=limit_mib * 1024 * 1024)


def whole(shape):
    return pl.BlockSpec(shape, lambda *_: (0,) * len(shape))


def pack_kernel(gate_ref, up_ref, down_ref, gu_ref, d_ref):
    mem = gate_ref.shape[0]

    def flat(ref):
        return [ref[m].astype(F32) for m in range(mem)]

    gu_ref[0] = jnp.concatenate(flat(gate_ref) + flat(up_ref), axis=0).astype(BF16)
    d_ref[0] = jnp.concatenate(flat(down_ref), axis=0).astype(BF16)


def pack_factors(gate, up, down, count):
    mem, rank, hidden = gate.shape
    part = hidden // count
    rows = mem * rank
    spec = pl.BlockSpec((mem, rank, part), lambda i: (0, 0, i))
    return pl.pallas_call(
        pack_kernel,
        grid=(count,),
        in_specs=[spec] * 3,
        out_specs=[
            pl.BlockSpec((1, 2 * rows, part), lambda i: (i, 0, 0)),
            pl.BlockSpec((1, rows, part), lambda i: (i, 0, 0)),
        ],
        out_shape=[
            jax.ShapeDtypeStruct((count, 2 * rows, part), BF16),
            jax.ShapeDtypeStruct((count, rows, part), BF16),
        ],
        compiler_params=compiler_params(16),
        name="pack_factors",
    )(gate, up, down)


def gate_up_kernel(shifts, z_count, hid_count, mem_local, *refs):
    blocks = len(shifts)
    pieces = refs[: PLANE * blocks]
    gw_ref, uw_ref, gif_ref, uif_ref = refs[PLANE * blocks : PLANE * blocks + 4]
    sends = refs[PLANE * blocks + 4 : PLANE * blocks + 3 + hid_count]
    keep_ref, keep_proj_ref, rows_ref = refs[PLANE * blocks + 3 + hid_count :]
    j = pl.program_id(0)
    z, x, c, y = place()
    units = PLANE * mem_local * blocks
    per_part = units // hid_count
    part_rows = per_part * SAMPLE_LENGTH
    columns = gw_ref.shape[1]
    hidden = keep_ref.shape[1] // 2

    @pl.when(j == 0)
    def _():
        for b in range(blocks):
            for q in range(PLANE):
                rx, rc = q % 2, q // 2
                piece = pieces[b * PLANE + q]
                slot = b * PLANE + jnp.bitwise_xor(x, rx) * CORE_COUNT + jnp.bitwise_xor(c, rc)
                for m in range(mem_local):
                    unit = slot * mem_local + m
                    part = unit // per_part
                    rel = lax.rem(part - y - 1 + hid_count, hid_count)
                    row = (rel * per_part + unit % per_part) * SAMPLE_LENGTH
                    rows_ref[pl.ds(pl.multiple_of(row, SAMPLE_LENGTH), SAMPLE_LENGTH), :] = piece[
                        m * SAMPLE_LENGTH : (m + 1) * SAMPLE_LENGTH, :
                    ]
        members = []
        for p in range(units):
            part = lax.rem(p // per_part + y + 1, hid_count)
            unit = part * per_part + p % per_part
            zs = jnp.int32(0)
            for b in range(blocks):
                zs = jnp.where(unit // (PLANE * mem_local) == b, lax.rem(z + shifts[b], z_count), zs)
            members.append(zs * PLANE * mem_local + unit % (PLANE * mem_local))
        rows = rows_ref[...]
        total = jnp.zeros((rows.shape[0], LANES), F32)
        for index, ref in enumerate((gif_ref, uif_ref)):
            projected = dot_nt(rows, ref[...])
            mine = row_members(projected.shape, members) == iota(projected.shape, 1) // RANK
            masked = jnp.where(mine, projected, 0.0)
            shape = (projected.shape[1], LANES)
            for level, value in enumerate(split_high_low(masked)):
                lane = iota(shape, 0) % RANK + RANK * (2 * index + level)
                pick = (lane == iota(shape, 1)).astype(F32).astype(BF16)
                total = total + dot(value, pick)
        packed = total.astype(BF16)
        for s in range(hid_count - 1):
            sends[s][:, 2 * hidden :] = packed[s * part_rows : (s + 1) * part_rows]
        keep_proj_ref[...] = packed[(hid_count - 1) * part_rows :]

    rows = rows_ref[...]
    for index, ref in enumerate((gw_ref, uw_ref)):
        value = dot(rows, ref[...])
        at = pl.ds(pl.multiple_of(index * hidden + j * columns, LANES), columns)
        for s in range(hid_count - 1):
            sends[s][:, at] = value[s * part_rows : (s + 1) * part_rows].astype(BF16)
        keep_ref[:, at] = value[(hid_count - 1) * part_rows :]


def gate_up(pieces, gw, uw, gif, uif, shifts, z_count, hid_count):
    rows, width = pieces[0].shape
    hidden = gw.shape[1]
    blocks = len(shifts)
    total = rows * PLANE * blocks
    part = total // hid_count
    columns = min(256, hidden)
    weight = pl.BlockSpec((width, columns), lambda j: (0, j))
    send_shape = (part, 2 * hidden + LANES)
    return pl.pallas_call(
        functools.partial(
            gate_up_kernel, shifts, z_count, hid_count, rows // SAMPLE_LENGTH
        ),
        grid=(hidden // columns,),
        in_specs=[whole((rows, width))] * len(pieces)
        + [weight, weight, whole(gif.shape), whole(uif.shape)],
        out_specs=[whole(send_shape)] * (hid_count - 1)
        + [whole((part, 2 * hidden)), whole((part, LANES))],
        out_shape=[jax.ShapeDtypeStruct(send_shape, BF16)] * (hid_count - 1)
        + [
            jax.ShapeDtypeStruct((part, 2 * hidden), F32),
            jax.ShapeDtypeStruct((part, LANES), BF16),
        ],
        scratch_shapes=[pltpu.VMEM((total, width), BF16)],
        compiler_params=compiler_params(32),
        cost_estimate=pl.CostEstimate(
            flops=4 * total * width * hidden, bytes_accessed=4 * width * hidden, transcendentals=0
        ),
        name="gate_up",
    )(*pieces, gw, uw, gif, uif)


def hidden_kernel(shifts, z_count, hid_count, mem_local, scale, *refs):
    blocks = len(shifts)
    keep_gate, keep_up, keep_proj = refs[:3]
    others = hid_count - 1
    recv_gate = refs[3 : 3 + others]
    recv_up = refs[3 + others : 3 + 2 * others]
    recv_proj = refs[3 + 2 * others : 3 + 3 * others]
    cols_ref, out_ref, proj_ref = refs[3 + 3 * others :]
    j = pl.program_id(0)
    z, x, c, y = place()
    per_part = PLANE * mem_local * blocks // hid_count
    lanes = cols_ref.shape[0]

    @pl.when(j == 0)
    def _():
        members = []
        for w in range(per_part):
            unit = y * per_part + w
            zs = jnp.int32(0)
            for b in range(blocks):
                zs = jnp.where(unit // (PLANE * mem_local) == b, lax.rem(z + shifts[b], z_count), zs)
            members.append(zs * PLANE * mem_local + unit % (PLANE * mem_local))
        rows = keep_proj.shape[0]
        lane = iota((rows, lanes), 1)
        group = mem_local * RANK
        member = lane // (2 * group) * mem_local + lane % group // RANK
        mine = row_members((rows, lanes), members) == member
        for index in range(2):
            source = iota((LANES, lanes), 0)
            target = iota((LANES, lanes), 1)
            base = target % RANK + 2 * RANK * index
            hit = (target // group % 2 == index) & ((source == base) | (source == base + RANK))
            spread = hit.astype(F32).astype(BF16)
            value = dot(keep_proj[...], spread)
            for ref in recv_proj:
                value = value + dot(ref[...], spread)
            high, low = split_high_low(jnp.where(mine, value, 0.0) * scale)
            proj_ref[2 * index] = high
            proj_ref[2 * index + 1] = low

    cols = cols_ref[...]

    def total(index, keep, recvs):
        value = keep[...]
        for ref in recvs:
            value = value + ref[...].astype(F32)
        return value + (dot(proj_ref[2 * index], cols) + dot(proj_ref[2 * index + 1], cols))

    gate = total(0, keep_gate, recv_gate)
    up = total(1, keep_up, recv_up)
    out_ref[...] = (gate / (1.0 + jnp.exp(-gate)) * up).astype(BF16)


def make_hidden(keep, keep_proj, recvs, cols, shifts, z_count, hid_count, mem_local, scale):
    part = keep.shape[0]
    hidden = keep.shape[1] // 2
    columns = min(256, hidden)
    steps = hidden // columns
    gate = pl.BlockSpec((part, columns), lambda j: (0, j))
    up = pl.BlockSpec((part, columns), lambda j: (0, steps + j))
    proj = pl.BlockSpec((part, LANES), lambda j: (0, 2 * hidden // LANES))
    lanes = cols.shape[0]
    return pl.pallas_call(
        functools.partial(hidden_kernel, shifts, z_count, hid_count, mem_local, scale),
        grid=(steps,),
        in_specs=[gate, up, whole((part, LANES))]
        + [gate] * len(recvs)
        + [up] * len(recvs)
        + [proj] * len(recvs)
        + [pl.BlockSpec((lanes, columns), lambda j: (0, j))],
        out_specs=gate,
        out_shape=jax.ShapeDtypeStruct((part, hidden), BF16),
        scratch_shapes=[pltpu.VMEM((4, part, lanes), BF16)],
        compiler_params=compiler_params(16),
        cost_estimate=pl.CostEstimate(
            flops=8 * part * lanes * hidden, bytes_accessed=8 * part * hidden, transcendentals=0
        ),
        name="make_hidden",
    )(keep, keep, keep_proj, *recvs, *recvs, *recvs, cols)


def down_kernel(shifts, z_count, hid_count, mem_local, scale, *refs):
    blocks = len(shifts)
    parts = refs[:hid_count]
    dw_ref, cols_ref, right_ref, send_ref, keep_ref, rows_ref, proj_ref = refs[hid_count:]
    j = pl.program_id(0)
    z, x, c, y = place()
    units = PLANE * mem_local * blocks
    per_part = units // hid_count
    half = send_ref.shape[0]

    @pl.when(j == 0)
    def _():
        for s in range(hid_count):
            for w in range(per_part):
                unit = lax.rem(y + s, hid_count) * per_part + w
                b = unit // (PLANE * mem_local)
                rx = jnp.bitwise_xor(unit // (CORE_COUNT * mem_local) % X_COUNT, x)
                rc = jnp.bitwise_xor(unit // mem_local % CORE_COUNT, c)
                slot = ((1 - rc) * X_COUNT + 1 - rx) * blocks + b
                row = (slot * mem_local + unit % mem_local) * SAMPLE_LENGTH
                rows_ref[pl.ds(pl.multiple_of(row, SAMPLE_LENGTH), SAMPLE_LENGTH), :] = parts[s][
                    w * SAMPLE_LENGTH : (w + 1) * SAMPLE_LENGTH, :
                ]
        members = []
        for p in range(units):
            slot, m = p // mem_local, p % mem_local
            q, b = slot // blocks, slot % blocks
            xs = jnp.bitwise_xor(x, 1 - q % X_COUNT)
            cs = jnp.bitwise_xor(c, 1 - q // X_COUNT)
            zs = lax.rem(z + shifts[b], z_count)
            members.append(((zs * X_COUNT + xs) * CORE_COUNT + cs) * mem_local + m)
        projected = dot_nt(rows_ref[...], cols_ref[...])
        mine = row_members(projected.shape, members) == iota(projected.shape, 1) // RANK
        high, low = split_high_low(jnp.where(mine, projected, 0.0) * scale)
        proj_ref[0] = high
        proj_ref[1] = low

    right = right_ref[...]
    value = dot(rows_ref[...], dw_ref[...]) + (dot(proj_ref[0], right) + dot(proj_ref[1], right))
    send_ref[...] = value[:half].astype(BF16)
    keep_ref[...] = value[half:]


def down(parts, dw, cols, right, shifts, z_count, hid_count, mem_local, scale):
    part, hidden = parts[0].shape
    width = dw.shape[1]
    total = part * hid_count
    columns = min(512, width)
    lanes = cols.shape[0]
    out = pl.BlockSpec((total // 2, columns), lambda j: (0, j))
    return pl.pallas_call(
        functools.partial(down_kernel, shifts, z_count, hid_count, mem_local, scale),
        grid=(width // columns,),
        in_specs=[whole((part, hidden))] * hid_count
        + [
            pl.BlockSpec((hidden, columns), lambda j: (0, j)),
            whole((lanes, hidden)),
            pl.BlockSpec((lanes, columns), lambda j: (0, j)),
        ],
        out_specs=[out, out],
        out_shape=[
            jax.ShapeDtypeStruct((total // 2, width), BF16),
            jax.ShapeDtypeStruct((total // 2, width), F32),
        ],
        scratch_shapes=[pltpu.VMEM((total, hidden), BF16), pltpu.VMEM((2, total, lanes), BF16)],
        compiler_params=compiler_params(32),
        cost_estimate=pl.CostEstimate(
            flops=2 * total * width * hidden, bytes_accessed=2 * width * hidden, transcendentals=0
        ),
        name="down",
    )(*parts, dw, cols, right)


def input_step_kernel(index, group, factor, fit_ref, in_ref, cols_ref, out_ref):
    scaled = (in_ref[...].astype(F32).T * fit_ref[...]).astype(BF16)
    shape = (scaled.shape[1], cols_ref.shape[0])
    source, target = iota(shape, 0), iota(shape, 1)
    hit = (target // group % 2 == index) & (
        target // (2 * group) * group + target % group == source
    )
    spread = dot(scaled, hit.astype(F32).astype(BF16)).astype(BF16)
    out_ref[...] = factor * dot(spread, cols_ref[...])


def input_step(index, group, factor, fit, in_factor, cols):
    lanes, width = in_factor.shape
    hidden = cols.shape[1]
    rows = min(256, width)
    return pl.pallas_call(
        functools.partial(input_step_kernel, index, group, factor),
        grid=(width // rows,),
        in_specs=[
            whole(fit.shape),
            pl.BlockSpec((lanes, rows), lambda i: (0, i)),
            whole(cols.shape),
        ],
        out_specs=pl.BlockSpec((rows, hidden), lambda i: (i, 0)),
        out_shape=jax.ShapeDtypeStruct((width, hidden), F32),
        compiler_params=compiler_params(24),
        cost_estimate=pl.CostEstimate(
            flops=2 * width * cols.shape[0] * hidden,
            bytes_accessed=4 * width * hidden,
            transcendentals=0,
        ),
        name=f"input_step_{index}",
    )(fit, in_factor, cols)


def down_step_kernel(factor, fit_ref, cols_ref, right_ref, out_ref, scaled_ref):
    @pl.when(pl.program_id(0) == 0)
    def _():
        scaled_ref[...] = (right_ref[...].astype(F32) * fit_ref[...]).astype(BF16)

    left = cols_ref[...].astype(F32).T.astype(BF16)
    out_ref[...] = factor * dot(left, scaled_ref[...])


def down_step(factor, fit_column, cols, right):
    lanes, hidden = cols.shape
    width = right.shape[1]
    rows = min(128, hidden)
    return pl.pallas_call(
        functools.partial(down_step_kernel, factor),
        grid=(hidden // rows,),
        in_specs=[
            whole(fit_column.shape),
            pl.BlockSpec((lanes, rows), lambda i: (0, i)),
            whole(right.shape),
        ],
        out_specs=pl.BlockSpec((rows, width), lambda i: (i, 0)),
        out_shape=jax.ShapeDtypeStruct((hidden, width), F32),
        scratch_shapes=[pltpu.VMEM(right.shape, BF16)],
        compiler_params=compiler_params(24),
        cost_estimate=pl.CostEstimate(
            flops=2 * width * lanes * hidden, bytes_accessed=4 * width * hidden, transcendentals=0
        ),
        name="down_step",
    )(fit_column, cols, right)


def local(
    tokens,
    fitness_ranks,
    gate_weight,
    up_weight,
    down_weight,
    gate_input_factor,
    up_input_factor,
    down_right,
    gate_output_factor,
    up_output_factor,
    down_left,
):
    pop_count = lax.axis_size("pop")
    hid_count = lax.axis_size("hid")
    z_count = pop_count // PLANE
    tok_local, width = tokens.shape
    mem_local = tok_local // SAMPLE_LENGTH
    members = mem_local * pop_count
    lanes = members * RANK
    hidden = gate_weight.shape[1]
    scale_in = 0.5 / math.sqrt(MODEL_WIDTH * RANK)
    scale_out = 0.5 / math.sqrt(HIDDEN_UNITS * RANK)
    factor = 1.0 / math.sqrt(members * RANK)

    everyone = range(pop_count)
    core_pairs = [(i, i ^ 1) for i in everyone]
    x_pairs = [(i, i ^ CORE_COUNT) for i in everyone]

    def forward(k):
        return [(i, (i + k * PLANE) % pop_count) for i in everyone]

    def along(v, pairs):
        return lax.ppermute(v, "pop", pairs)

    groups = [(k,) for k in range(z_count)]

    blocks = {}
    for k in range(z_count):
        own = tokens if k == 0 else along(tokens, forward(z_count - k))
        from_x = along(own, x_pairs)
        from_core = along(own, core_pairs)
        blocks[k] = [own, from_x, from_core, along(from_x, core_pairs)]

    gif = gate_input_factor.reshape(lanes, width)
    uif = up_input_factor.reshape(lanes, width)
    right = down_right.reshape(lanes, width)
    gu_sent, d_sent = pack_factors(gate_output_factor, up_output_factor, down_left, pop_count)
    gu_cols = lax.all_to_all(gu_sent, "pop", split_axis=0, concat_axis=0, tiled=True)
    gu_cols = gu_cols.reshape(2 * lanes, hidden)
    d_cols = lax.all_to_all(d_sent, "pop", split_axis=0, concat_axis=0, tiled=True)
    d_cols = d_cols.reshape(lanes, hidden)

    total = None
    for shifts in groups:
        pieces = [piece for k in shifts for piece in blocks[k]]
        *sends, keep, keep_proj = gate_up(
            pieces, gate_weight, up_weight, gif, uif, shifts, z_count, hid_count
        )
        recvs = [
            lax.ppermute(v, "hid", [(i, (i + s + 1) % hid_count) for i in range(hid_count)])
            for s, v in enumerate(sends)
        ]
        mine = make_hidden(
            keep, keep_proj, recvs, gu_cols, shifts, z_count, hid_count, mem_local, scale_in
        )
        parts = [mine] + [
            lax.ppermute(mine, "hid", [((i + s) % hid_count, i) for i in range(hid_count)])
            for s in range(1, hid_count)
        ]
        send, held = down(
            parts, down_weight, d_cols, right, shifts, z_count, hid_count, mem_local, scale_out
        )
        held = held + along(send, core_pairs).astype(F32)
        half = held.shape[0] // 2
        held = held[half:] + along(held[:half].astype(BF16), x_pairs).astype(F32)
        for b, k in enumerate(shifts):
            piece = held[b * tok_local : (b + 1) * tok_local]
            if k:
                piece = along(piece.astype(BF16), forward(k)).astype(F32)
            total = piece if total is None else total + piece
    mixed = total.astype(BF16)

    fit = jnp.repeat(fitness_ranks.astype(F32) / (members - 1) - 0.5, RANK)
    group = mem_local * RANK
    gate_step = input_step(0, group, factor, fit[None, :], gif, gu_cols)
    up_step = input_step(1, group, factor, fit[None, :], uif, gu_cols)
    step = down_step(factor, fit[:, None], d_cols, right)
    return (mixed, gate_step, up_step, step)


def solution(mesh):
    in_specs = (
        P("pop", "hid"),
        P(),
        P("hid", "pop"),
        P("hid", "pop"),
        P("pop", "hid"),
        P(None, None, "hid"),
        P(None, None, "hid"),
        P(None, None, "hid"),
        P("pop", None, None),
        P("pop", None, None),
        P("pop", None, None),
    )
    out_specs = (P("pop", "hid"), P("hid", "pop"), P("hid", "pop"), P("pop", "hid"))
    return jax.shard_map(local, mesh=mesh, in_specs=in_specs, out_specs=out_specs, check_vma=False)
```

```python
import functools
import math

import jax
import jax.numpy as jnp
from jax import lax
from jax.experimental import pallas as pl
from jax.experimental.pallas import tpu as pltpu
from jax.sharding import PartitionSpec as P


MODEL_WIDTH = 4096
HIDDEN_UNITS = 16384
RANK = 4
SAMPLE_LENGTH = 16
X_COUNT = 2
CORE_COUNT = 2
PLANE = X_COUNT * CORE_COUNT
LANES = 128
F32 = jnp.float32
BF16 = jnp.bfloat16


def dot(a, b):
    return jnp.dot(a, b, preferred_element_type=F32)


def dot_nt(a, b):
    return lax.dot_general(a, b, (((1,), (1,)), ((), ())), preferred_element_type=F32)


def split_high_low(v):
    high = v.astype(BF16)
    return high, (v - high.astype(F32)).astype(BF16)


def place():
    p = lax.axis_index("pop")
    y = lax.axis_index("hid")
    return p // PLANE, (p // CORE_COUNT) % X_COUNT, p % CORE_COUNT, y


def iota(shape, dim):
    return lax.broadcasted_iota(jnp.int32, shape, dim)


def row_members(shape, members):
    unit = iota(shape, 0) // SAMPLE_LENGTH
    out = jnp.zeros(shape, jnp.int32)
    for index, member in enumerate(members):
        out = jnp.where(unit == index, member, out)
    return out


def compiler_params(limit_mib):
    return pltpu.CompilerParams(vmem_limit_bytes=limit_mib * 1024 * 1024)


IN_VMEM = pl.BlockSpec(memory_space=pltpu.VMEM)
IN_HBM = pl.BlockSpec(memory_space=pltpu.HBM)
IN_SMEM = pl.BlockSpec(memory_space=pltpu.SMEM)


def fixed(*arrays):
    return [pltpu.with_memory_space_constraint(v, pltpu.HBM) for v in arrays]


def fetch(pairs, sem):
    copies = [pltpu.make_async_copy(a, b, sem.at[i]) for i, (a, b) in enumerate(pairs)]
    for copy in copies:
        copy.start()
    return copies


def pack_kernel(z_count, gate_in, up_in, down_in, *refs):
    outs, parts, sem = refs[:PLANE], refs[PLANE : PLANE + 3], refs[PLANE + 3]
    for copy in fetch(zip((gate_in, up_in, down_in), parts), sem):
        copy.wait()
    z, x, c, _ = place()
    mem = parts[0].shape[0]
    part = outs[0].shape[2]
    for q in range(PLANE):
        xs, cs = jnp.bitwise_xor(x, q % X_COUNT), jnp.bitwise_xor(c, q // X_COUNT)
        for k in range(z_count):
            to = (lax.rem(z + k, z_count) * X_COUNT + xs) * CORE_COUNT + cs
            at = pl.ds(pl.multiple_of(to * part, LANES), part)
            rows = [ref[m, :, at].astype(F32) for ref in parts for m in range(mem)]
            outs[q][k] = jnp.concatenate(rows, axis=0).astype(BF16)


def pack(gate, up, down, z_count):
    mem, rank, hidden = gate.shape
    part = hidden // (z_count * PLANE)
    return pl.pallas_call(
        functools.partial(pack_kernel, z_count),
        in_specs=[IN_HBM] * 3,
        out_specs=[IN_VMEM] * PLANE,
        out_shape=[jax.ShapeDtypeStruct((z_count, 3 * mem * rank, part), BF16)] * PLANE,
        scratch_shapes=[pltpu.VMEM(gate.shape, BF16)] * 3 + [pltpu.SemaphoreType.DMA((3,))],
        compiler_params=compiler_params(8),
        cost_estimate=pl.CostEstimate(
            flops=512 * gate.size, bytes_accessed=12 * gate.size, transcendentals=0
        ),
        name="pack",
    )(*fixed(gate, up, down))


def merge_kernel(*refs):
    ins, outs, rows_ref = refs[:PLANE], refs[PLANE:-1], refs[-1]
    _, x, c, _ = place()
    group = ins[0].shape[1] // 3
    tall = 2 * group
    for k, out in enumerate(outs):
        for q in range(PLANE):
            xs, cs = jnp.bitwise_xor(x, q % X_COUNT), jnp.bitwise_xor(c, q // X_COUNT)
            slot = xs * CORE_COUNT + cs
            out[pl.ds(pl.multiple_of(slot * tall, tall), tall), :] = ins[q][k, :tall, :]
            rows_ref[pl.ds(pl.multiple_of(slot * group, group), group), :] = ins[q][
                k, tall:, :
            ].astype(F32)
        out[PLANE * tall :, :] = rows_ref[...].astype(BF16)


def merge(blocks):
    z_count, rows, part = blocks[0].shape
    return pl.pallas_call(
        merge_kernel,
        in_specs=[IN_VMEM] * PLANE,
        out_specs=[IN_VMEM] * z_count,
        out_shape=[jax.ShapeDtypeStruct((PLANE * rows, part), BF16)] * z_count,
        scratch_shapes=[pltpu.VMEM((PLANE * rows // 3, part), F32)],
        compiler_params=compiler_params(8),
        cost_estimate=pl.CostEstimate(
            flops=512 * z_count * rows * part, bytes_accessed=16 * rows * part, transcendentals=0
        ),
        name="merge",
    )(*blocks)


def load_kernel(mem, gif_in, uif_in, gw_in, uw_in, giu_ref, gw_ref, uw_ref, gif_ref, uif_ref, sem):
    copies = fetch(
        ((gif_in, gif_ref), (uif_in, uif_ref), (gw_in, gw_ref), (uw_in, uw_ref)), sem
    )
    for copy in copies[:2]:
        copy.wait()
    tall = 2 * mem * RANK
    for p in range(gif_ref.shape[0] // mem):
        rows = [ref[p * mem + m].astype(F32) for ref in (gif_ref, uif_ref) for m in range(mem)]
        giu_ref[p * tall : (p + 1) * tall] = jnp.concatenate(rows, axis=0).astype(BF16)
    for copy in copies[2:]:
        copy.wait()


def load(gif, uif, gw, uw, mem):
    members, rank, width = gif.shape
    return pl.pallas_call(
        functools.partial(load_kernel, mem),
        in_specs=[IN_HBM] * 4,
        out_specs=[IN_VMEM] * 3,
        out_shape=[
            pltpu.VMEM((2 * members * rank, width), BF16),
            pltpu.VMEM(gw.shape, BF16),
            pltpu.VMEM(uw.shape, BF16),
        ],
        scratch_shapes=[pltpu.VMEM(gif.shape, BF16)] * 2 + [pltpu.SemaphoreType.DMA((4,))],
        compiler_params=compiler_params(16),
        cost_estimate=pl.CostEstimate(
            flops=1024 * gw.size, bytes_accessed=4 * gw.size, transcendentals=0
        ),
        name="load",
    )(*fixed(gif, uif, gw, uw))


def scaled(ranks_ref, members, value, first, number):
    member = iota((value.shape[0], 1), 0) // RANK % number
    rank = jnp.zeros(member.shape, jnp.int32)
    for m in range(number):
        rank = jnp.where(member == m, ranks_ref[first + m], rank)
    return (value * (rank.astype(F32) / (members - 1) - 0.5)).astype(BF16)


def turn_into(out_ref, in_ref):
    columns = min(256, in_ref.shape[1])
    for j in range(in_ref.shape[1] // columns):
        at = slice(j * columns, (j + 1) * columns)
        out_ref[at] = in_ref[:, at].T.astype(BF16)


def turn_kernel(mem, ranks_ref, gif_in, uif_in, out_ref, gif_ref, uif_ref, rows_ref, sem):
    for copy in fetch(((gif_in, gif_ref), (uif_in, uif_ref)), sem):
        copy.wait()
    members = gif_ref.shape[0]
    tall = 2 * mem * RANK
    for p in range(members // mem):
        pieces = [ref[p * mem + m].astype(F32) for ref in (gif_ref, uif_ref) for m in range(mem)]
        value = scaled(ranks_ref, members, jnp.concatenate(pieces, axis=0), p * mem, mem)
        rows_ref[p * tall : (p + 1) * tall] = value.astype(F32)
    turn_into(out_ref, rows_ref)


def turn(ranks, gif, uif, mem):
    members, rank, width = gif.shape
    lanes = 2 * members * rank
    return pl.pallas_call(
        functools.partial(turn_kernel, mem),
        in_specs=[IN_SMEM] + [IN_HBM] * 2,
        out_specs=IN_VMEM,
        out_shape=jax.ShapeDtypeStruct((width, lanes), BF16),
        scratch_shapes=[pltpu.VMEM(gif.shape, BF16)] * 2
        + [pltpu.VMEM((lanes, width), F32), pltpu.SemaphoreType.DMA((2,))],
        compiler_params=compiler_params(12),
        cost_estimate=pl.CostEstimate(
            flops=4096 * gif.size, bytes_accessed=8 * gif.size, transcendentals=0
        ),
        name="turn",
    )(ranks, *fixed(gif, uif))


def arrange_kernel(z_count, ranks_ref, right_in, dw_in, *refs):
    gots = refs[:z_count]
    gu_ref, d_ref, dt_ref, right_ref, sright_ref, dw_ref = refs[z_count : z_count + 6]
    raw_ref, rows_ref, sem = refs[z_count + 6 :]
    copies = fetch(((right_in, raw_ref), (dw_in, dw_ref)), sem)
    z, _, _, _ = place()
    third = gots[0].shape[0] // 3
    members = raw_ref.shape[0]
    for k, got in enumerate(gots):
        zs = lax.rem(z - k + z_count, z_count)
        gu_ref[pl.ds(pl.multiple_of(zs * 2 * third, 2 * third), 2 * third), :] = got[: 2 * third, :]
        down_at = pl.ds(pl.multiple_of(zs * third, third), third)
        d_ref[down_at, :] = got[2 * third :, :]
        rows_ref[down_at, :] = got[2 * third :, :].astype(F32)
    turn_into(dt_ref, rows_ref)
    copies[0].wait()
    number = 4
    tall = number * RANK
    for p in range(members // number):
        value = jnp.concatenate([raw_ref[p * number + m].astype(F32) for m in range(number)], axis=0)
        right_ref[p * tall : (p + 1) * tall] = value.astype(BF16)
        sright_ref[p * tall : (p + 1) * tall] = scaled(ranks_ref, members, value, p * number, number)
    copies[1].wait()


def arrange(ranks, gots, right, dw):
    hidden = gots[0].shape[1]
    members, rank, width = right.shape
    lanes = members * rank
    return pl.pallas_call(
        functools.partial(arrange_kernel, len(gots)),
        in_specs=[IN_SMEM] + [IN_HBM] * 2 + [IN_VMEM] * len(gots),
        out_specs=[IN_VMEM] * 6,
        out_shape=[
            pltpu.VMEM((2 * lanes, hidden), BF16),
            pltpu.VMEM((lanes, hidden), BF16),
            pltpu.VMEM((hidden, lanes), BF16),
            pltpu.VMEM((lanes, width), BF16),
            pltpu.VMEM((lanes, width), BF16),
            pltpu.VMEM(dw.shape, BF16),
        ],
        scratch_shapes=[
            pltpu.VMEM(right.shape, BF16),
            pltpu.VMEM((lanes, hidden), F32),
            pltpu.SemaphoreType.DMA((2,)),
        ],
        compiler_params=compiler_params(16),
        cost_estimate=pl.CostEstimate(
            flops=1024 * dw.size, bytes_accessed=4 * dw.size, transcendentals=0
        ),
        name="arrange",
    )(ranks, *fixed(right, dw), *gots)


def unit_members(units, per_block, shifts, z, z_count, start):
    members = []
    for w in range(units):
        unit = start(w)
        zs = jnp.int32(0)
        for b, shift in enumerate(shifts):
            zs = jnp.where(unit // per_block == b, lax.rem(z + shift, z_count), zs)
        members.append(zs * per_block + unit % per_block)
    return members


def lane_members(shape, group):
    lane = iota(shape, 1)
    return lane // (2 * group) * (group // RANK) + lane % group // RANK


def gate_up_kernel(shifts, z_count, hid_count, mem_local, *refs):
    blocks = len(shifts)
    pieces = refs[: PLANE * blocks]
    gw_ref, uw_ref, giu_ref = refs[PLANE * blocks : PLANE * blocks + 3]
    sends = refs[PLANE * blocks + 3 : PLANE * blocks + 2 + hid_count]
    keep_ref, keep_proj_ref, rows_ref = refs[PLANE * blocks + 2 + hid_count :]
    z, x, c, y = place()
    per_block = PLANE * mem_local
    units = per_block * blocks
    per_part = units // hid_count
    part_rows = per_part * SAMPLE_LENGTH
    hidden = keep_ref.shape[1] // 2
    columns = min(256, hidden)
    group = mem_local * RANK
    for b in range(blocks):
        for q in range(PLANE):
            rx, rc = q % 2, q // 2
            piece = pieces[b * PLANE + q]
            slot = b * PLANE + jnp.bitwise_xor(x, rx) * CORE_COUNT + jnp.bitwise_xor(c, rc)
            for m in range(mem_local):
                unit = slot * mem_local + m
                rel = lax.rem(unit // per_part - y - 1 + hid_count, hid_count)
                row = (rel * per_part + unit % per_part) * SAMPLE_LENGTH
                rows_ref[pl.ds(pl.multiple_of(row, SAMPLE_LENGTH), SAMPLE_LENGTH), :] = piece[
                    m * SAMPLE_LENGTH : (m + 1) * SAMPLE_LENGTH, :
                ]
    members = unit_members(
        units,
        per_block,
        shifts,
        z,
        z_count,
        lambda p: lax.rem(p // per_part + y + 1, hid_count) * per_part + p % per_part,
    )
    rows = rows_ref[...]
    projected = dot_nt(rows, giu_ref[...])
    mine = row_members(projected.shape, members) == lane_members(projected.shape, group)
    high, low = split_high_low(jnp.where(mine, projected, 0.0))
    shape = (projected.shape[1], LANES)
    lane = iota(shape, 0) % RANK + 2 * RANK * (iota(shape, 0) // group % 2)

    def pick(level):
        return (lane + RANK * level == iota(shape, 1)).astype(F32).astype(BF16)

    packed = (dot(high, pick(0)) + dot(low, pick(1))).astype(BF16)
    for s in range(hid_count - 1):
        sends[s][:, 2 * hidden :] = packed[s * part_rows : (s + 1) * part_rows]
    keep_proj_ref[...] = packed[(hid_count - 1) * part_rows :]
    for j in range(hidden // columns):
        for index, ref in enumerate((gw_ref, uw_ref)):
            value = dot(rows, ref[:, j * columns : (j + 1) * columns])
            at = slice(index * hidden + j * columns, index * hidden + (j + 1) * columns)
            for s in range(hid_count - 1):
                sends[s][:, at] = value[s * part_rows : (s + 1) * part_rows].astype(BF16)
            keep_ref[:, at] = value[(hid_count - 1) * part_rows :]


def gate_up(pieces, gw, uw, giu, shifts, z_count, hid_count):
    rows, width = pieces[0].shape
    hidden = gw.shape[1]
    total = rows * PLANE * len(shifts)
    part = total // hid_count
    send_shape = (part, 2 * hidden + LANES)
    return pl.pallas_call(
        functools.partial(
            gate_up_kernel, shifts, z_count, hid_count, rows // SAMPLE_LENGTH
        ),
        in_specs=[IN_VMEM] * (len(pieces) + 3),
        out_specs=[IN_VMEM] * (hid_count + 1),
        out_shape=[jax.ShapeDtypeStruct(send_shape, BF16)] * (hid_count - 1)
        + [
            jax.ShapeDtypeStruct((part, 2 * hidden), F32),
            jax.ShapeDtypeStruct((part, LANES), BF16),
        ],
        scratch_shapes=[pltpu.VMEM((total, width), BF16)],
        compiler_params=compiler_params(24),
        cost_estimate=pl.CostEstimate(
            flops=4 * total * width * hidden, bytes_accessed=4 * width * hidden, transcendentals=0
        ),
        name="gate_up",
    )(*pieces, gw, uw, giu)


def hidden_kernel(shifts, z_count, hid_count, mem_local, scale, *refs):
    keep_ref, keep_proj = refs[:2]
    recvs = refs[2 : 1 + hid_count]
    cols_ref, out_ref = refs[1 + hid_count :]
    z, _, _, y = place()
    per_block = PLANE * mem_local
    per_part = per_block * len(shifts) // hid_count
    lanes, hidden = cols_ref.shape
    group = mem_local * RANK
    rows = keep_proj.shape[0]
    members = unit_members(
        per_part, per_block, shifts, z, z_count, lambda w: y * per_part + w
    )
    mine = row_members((rows, lanes), members) == lane_members((rows, lanes), group)
    source, target = iota((LANES, lanes), 0), iota((LANES, lanes), 1)
    base = target % RANK + 2 * RANK * (target // group % 2)
    spread = ((source == base) | (source == base + RANK)).astype(F32).astype(BF16)
    value = dot(keep_proj[...], spread)
    for ref in recvs:
        value = value + dot(ref[:, 2 * hidden :], spread)
    value = jnp.where(mine, value, 0.0) * scale
    of_gate = iota((rows, lanes), 1) // group % 2 == 0
    gate_high, gate_low = split_high_low(jnp.where(of_gate, value, 0.0))
    up_high, up_low = split_high_low(jnp.where(of_gate, 0.0, value))
    stack = jnp.concatenate([gate_high, gate_low, up_high, up_low], axis=0)
    columns = min(256, hidden)
    for j in range(hidden // columns):
        lowrank = dot(stack, cols_ref[:, j * columns : (j + 1) * columns])

        def total(index):
            at = slice(index * hidden + j * columns, index * hidden + (j + 1) * columns)
            value = keep_ref[:, at]
            for ref in recvs:
                value = value + ref[:, at].astype(F32)
            first = 2 * index * rows
            return value + (lowrank[first : first + rows] + lowrank[first + rows : first + 2 * rows])

        gate, up = total(0), total(1)
        out_ref[:, j * columns : (j + 1) * columns] = (
            gate / (1.0 + jnp.exp(-gate)) * up
        ).astype(BF16)


def make_hidden(keep, keep_proj, recvs, cols, shifts, z_count, hid_count, mem_local, scale):
    part = keep.shape[0]
    hidden = keep.shape[1] // 2
    lanes = cols.shape[0]
    return pl.pallas_call(
        functools.partial(hidden_kernel, shifts, z_count, hid_count, mem_local, scale),
        in_specs=[IN_VMEM] * (3 + len(recvs)),
        out_specs=IN_VMEM,
        out_shape=jax.ShapeDtypeStruct((part, hidden), BF16),
        compiler_params=compiler_params(12),
        cost_estimate=pl.CostEstimate(
            flops=8 * part * lanes * hidden, bytes_accessed=8 * part * hidden, transcendentals=0
        ),
        name="make_hidden",
    )(keep, keep_proj, *recvs, cols)


def down_kernel(shifts, z_count, hid_count, mem_local, scale, *refs):
    blocks = len(shifts)
    parts = refs[:hid_count]
    dw_ref, cols_ref, right_ref, send_ref, keep_ref, rows_ref = refs[hid_count:]
    z, x, c, y = place()
    units = PLANE * mem_local * blocks
    per_part = units // hid_count
    half, width = send_ref.shape
    for s in range(hid_count):
        for w in range(per_part):
            unit = lax.rem(y + s, hid_count) * per_part + w
            b = unit // (PLANE * mem_local)
            rx = jnp.bitwise_xor(unit // (CORE_COUNT * mem_local) % X_COUNT, x)
            rc = jnp.bitwise_xor(unit // mem_local % CORE_COUNT, c)
            slot = ((1 - rc) * X_COUNT + 1 - rx) * blocks + b
            row = (slot * mem_local + unit % mem_local) * SAMPLE_LENGTH
            rows_ref[pl.ds(pl.multiple_of(row, SAMPLE_LENGTH), SAMPLE_LENGTH), :] = parts[s][
                w * SAMPLE_LENGTH : (w + 1) * SAMPLE_LENGTH, :
            ]
    members = []
    for p in range(units):
        slot, m = p // mem_local, p % mem_local
        q, b = slot // blocks, slot % blocks
        xs = jnp.bitwise_xor(x, 1 - q % X_COUNT)
        cs = jnp.bitwise_xor(c, 1 - q // X_COUNT)
        zs = lax.rem(z + shifts[b], z_count)
        members.append(((zs * X_COUNT + xs) * CORE_COUNT + cs) * mem_local + m)
    rows = rows_ref[...]
    projected = dot_nt(rows, cols_ref[...])
    mine = row_members(projected.shape, members) == iota(projected.shape, 1) // RANK
    both = jnp.concatenate(split_high_low(jnp.where(mine, projected, 0.0) * scale), axis=1)
    columns = min(256, width)
    for j in range(width // columns):
        at = slice(j * columns, (j + 1) * columns)
        right = right_ref[:, at]
        value = dot(rows, dw_ref[:, at]) + dot(both, jnp.concatenate([right, right], axis=0))
        send_ref[:, at] = value[:half].astype(BF16)
        keep_ref[:, at] = value[half:]


def down(parts, dw, cols, right, shifts, z_count, hid_count, mem_local, scale):
    part, hidden = parts[0].shape
    width = dw.shape[1]
    total = part * hid_count
    return pl.pallas_call(
        functools.partial(down_kernel, shifts, z_count, hid_count, mem_local, scale),
        in_specs=[IN_VMEM] * (hid_count + 3),
        out_specs=[IN_VMEM] * 2,
        out_shape=[
            jax.ShapeDtypeStruct((total // 2, width), BF16),
            jax.ShapeDtypeStruct((total // 2, width), F32),
        ],
        scratch_shapes=[pltpu.VMEM((total, hidden), BF16)],
        compiler_params=compiler_params(16),
        cost_estimate=pl.CostEstimate(
            flops=2 * total * width * hidden, bytes_accessed=2 * width * hidden, transcendentals=0
        ),
        name="down",
    )(*parts, dw, cols, right)


def input_step_kernel(index, group, factor, in_ref, cols_ref, out_ref):
    rows = out_ref.shape[0]
    left = in_ref[pl.ds(pl.multiple_of(pl.program_id(0) * rows, LANES), rows), :]
    belongs = iota(left.shape, 1) // group % 2 == index
    left = jnp.where(belongs, left.astype(F32), 0.0).astype(BF16)
    out_ref[...] = factor * dot(left, cols_ref[...])


def input_step(index, group, factor, in_factor, cols):
    width, lanes = in_factor.shape
    hidden = cols.shape[1]
    rows = min(512, width)
    return pl.pallas_call(
        functools.partial(input_step_kernel, index, group, factor),
        grid=(width // rows,),
        in_specs=[IN_VMEM] * 2,
        out_specs=pl.BlockSpec((rows, hidden), lambda i: (i, 0)),
        out_shape=jax.ShapeDtypeStruct((width, hidden), F32),
        compiler_params=compiler_params(12),
        cost_estimate=pl.CostEstimate(
            flops=8 * width * lanes * hidden, bytes_accessed=4 * width * hidden, transcendentals=0
        ),
    )(in_factor, cols)


def down_step_kernel(factor, left_ref, right_ref, out_ref):
    rows = out_ref.shape[0]
    left = left_ref[pl.ds(pl.multiple_of(pl.program_id(0) * rows, LANES), rows), :]
    out_ref[...] = factor * dot(left, right_ref[...])


def down_step(factor, left, right):
    hidden, lanes = left.shape
    width = right.shape[1]
    rows = min(256, hidden)
    return pl.pallas_call(
        functools.partial(down_step_kernel, factor),
        grid=(hidden // rows,),
        in_specs=[IN_VMEM] * 2,
        out_specs=pl.BlockSpec((rows, width), lambda i: (i, 0)),
        out_shape=jax.ShapeDtypeStruct((hidden, width), F32),
        compiler_params=compiler_params(12),
        cost_estimate=pl.CostEstimate(
            flops=8 * width * lanes * hidden, bytes_accessed=4 * width * hidden, transcendentals=0
        ),
        name="down_step",
    )(left, right)


def local(
    tokens,
    fitness_ranks,
    gate_weight,
    up_weight,
    down_weight,
    gate_input_factor,
    up_input_factor,
    down_right,
    gate_output_factor,
    up_output_factor,
    down_left,
):
    pop_count = lax.axis_size("pop")
    hid_count = lax.axis_size("hid")
    z_count = pop_count // PLANE
    tok_local, _ = tokens.shape
    mem_local = tok_local // SAMPLE_LENGTH
    members = mem_local * pop_count
    scale_in = 0.5 / math.sqrt(MODEL_WIDTH * RANK)
    scale_out = 0.5 / math.sqrt(HIDDEN_UNITS * RANK)
    factor = 1.0 / math.sqrt(members * RANK)

    everyone = range(pop_count)
    core_pairs = [(i, i ^ 1) for i in everyone]
    x_pairs = [(i, i ^ CORE_COUNT) for i in everyone]

    def forward(k):
        return [(i, (i + k * PLANE) % pop_count) for i in everyone]

    def along(v, pairs):
        return lax.ppermute(v, "pop", pairs)

    groups = GROUPS(z_count)

    blocks = {}
    for k in range(z_count):
        own = tokens if k == 0 else along(tokens, forward(z_count - k))
        from_x = along(own, x_pairs)
        from_core = along(own, core_pairs)
        from_both = along(from_x, core_pairs)
        blocks[k] = [own, from_x, from_core, from_both]

    near, near_x, far, far_x = pack(gate_output_factor, up_output_factor, down_left, z_count)
    from_x = along(near_x, x_pairs)
    far_x = along(far_x, core_pairs)
    far = along(far, core_pairs)
    far_x = along(far_x, x_pairs)
    joined = merge([near, from_x, far, far_x])
    gots = []
    for k in range(z_count):
        gots.append(along(joined[k], forward(k)) if k else joined[k])
    giu, gate_v, up_v = load(gate_input_factor, up_input_factor, gate_weight, up_weight, mem_local)
    scaled_giu = turn(fitness_ranks, gate_input_factor, up_input_factor, mem_local)
    gu_cols, d_cols, d_turned, right, scaled_right, down_v = arrange(
        fitness_ranks, gots, down_right, down_weight
    )

    total = None
    for shifts in groups:
        pieces = [piece for k in shifts for piece in blocks[k]]
        *sends, keep, keep_proj = gate_up(
            pieces, gate_v, up_v, giu, shifts, z_count, hid_count
        )
        recvs = [
            lax.ppermute(v, "hid", [(i, (i + s + 1) % hid_count) for i in range(hid_count)])
            for s, v in enumerate(sends)
        ]
        mine = make_hidden(
            keep, keep_proj, recvs, gu_cols, shifts, z_count, hid_count, mem_local, scale_in
        )
        parts = [mine] + [
            lax.ppermute(mine, "hid", [((i + s) % hid_count, i) for i in range(hid_count)])
            for s in range(1, hid_count)
        ]
        send, held = down(
            parts, down_v, d_cols, right, shifts, z_count, hid_count, mem_local, scale_out
        )
        held = held + along(send, core_pairs).astype(F32)
        half = held.shape[0] // 2
        held = held[half:] + along(held[:half].astype(BF16), x_pairs).astype(F32)
        for b, k in enumerate(shifts):
            piece = held[b * tok_local : (b + 1) * tok_local]
            if k:
                piece = along(piece.astype(BF16), forward(k)).astype(F32)
            total = piece if total is None else total + piece
    mixed = total.astype(BF16)

    group = mem_local * RANK
    gate_step = input_step(0, group, factor, scaled_giu, gu_cols)
    up_step = input_step(1, group, factor, scaled_giu, gu_cols)
    step = down_step(factor, d_turned, scaled_right)
    return (mixed, gate_step, up_step, step)


def GROUPS(z_count):
    return [(1,), *[tuple(range(z_count))[i : i + 2] for i in range(2, z_count, 2)], (0,)]


def solution(mesh):
    in_specs = (
        P("pop", "hid"),
        P(),
        P("hid", "pop"),
        P("hid", "pop"),
        P("pop", "hid"),
        P(None, None, "hid"),
        P(None, None, "hid"),
        P(None, None, "hid"),
        P("pop", None, None),
        P("pop", None, None),
        P("pop", None, None),
    )
    out_specs = (P("pop", "hid"), P("hid", "pop"), P("hid", "pop"), P("pop", "hid"))
    return jax.shard_map(local, mesh=mesh, in_specs=in_specs, out_specs=out_specs, check_vma=False)
```

```python
import functools
import math

import jax
import jax.numpy as jnp
from jax import lax
from jax.experimental import pallas as pl
from jax.experimental.pallas import tpu as pltpu
from jax.sharding import PartitionSpec as P


MODEL_WIDTH = 4096
HIDDEN_UNITS = 16384
RANK = 4
SAMPLE_LENGTH = 16
X_COUNT = 2
CORE_COUNT = 2
PLANE = X_COUNT * CORE_COUNT
LANES = 128
F32 = jnp.float32
BF16 = jnp.bfloat16


def dot(a, b):
    return jnp.dot(a, b, preferred_element_type=F32)


def dot_nt(a, b):
    return lax.dot_general(a, b, (((1,), (1,)), ((), ())), preferred_element_type=F32)


def split_high_low(v):
    high = v.astype(BF16)
    return high, (v - high.astype(F32)).astype(BF16)


def place():
    p = lax.axis_index("pop")
    y = lax.axis_index("hid")
    return p // PLANE, (p // CORE_COUNT) % X_COUNT, p % CORE_COUNT, y


def iota(shape, dim):
    return lax.broadcasted_iota(jnp.int32, shape, dim)


def row_members(shape, members):
    unit = iota(shape, 0) // SAMPLE_LENGTH
    out = jnp.zeros(shape, jnp.int32)
    for index, member in enumerate(members):
        out = jnp.where(unit == index, member, out)
    return out


def compiler_params(limit_mib):
    return pltpu.CompilerParams(vmem_limit_bytes=limit_mib * 1024 * 1024)


IN_VMEM = pl.BlockSpec(memory_space=pltpu.VMEM)
IN_HBM = pl.BlockSpec(memory_space=pltpu.HBM)
IN_SMEM = pl.BlockSpec(memory_space=pltpu.SMEM)


def fixed(*arrays):
    return [pltpu.with_memory_space_constraint(v, pltpu.HBM) for v in arrays]


def fetch(pairs, sem):
    copies = [pltpu.make_async_copy(a, b, sem.at[i]) for i, (a, b) in enumerate(pairs)]
    for copy in copies:
        copy.start()
    return copies


def pack_kernel(z_count, gate_in, up_in, down_in, *refs):
    outs, parts, sem = refs[:PLANE], refs[PLANE : PLANE + 3], refs[PLANE + 3]
    for copy in fetch(zip((gate_in, up_in, down_in), parts), sem):
        copy.wait()
    z, x, c, _ = place()
    mem = parts[0].shape[0]
    part = outs[0].shape[2]
    for q in range(PLANE):
        xs, cs = jnp.bitwise_xor(x, q % X_COUNT), jnp.bitwise_xor(c, q // X_COUNT)
        for k in range(z_count):
            to = (jnp.bitwise_xor(z, k) * X_COUNT + xs) * CORE_COUNT + cs
            at = pl.ds(pl.multiple_of(to * part, LANES), part)
            rows = [ref[m, :, at].astype(F32) for ref in parts for m in range(mem)]
            outs[q][k] = jnp.concatenate(rows, axis=0).astype(BF16)


def pack(gate, up, down, z_count):
    mem, rank, hidden = gate.shape
    part = hidden // (z_count * PLANE)
    return pl.pallas_call(
        functools.partial(pack_kernel, z_count),
        in_specs=[IN_HBM] * 3,
        out_specs=[IN_VMEM] * PLANE,
        out_shape=[jax.ShapeDtypeStruct((z_count, 3 * mem * rank, part), BF16)] * PLANE,
        scratch_shapes=[pltpu.VMEM(gate.shape, BF16)] * 3 + [pltpu.SemaphoreType.DMA((3,))],
        compiler_params=compiler_params(8),
        cost_estimate=pl.CostEstimate(
            flops=512 * gate.size, bytes_accessed=12 * gate.size, transcendentals=0
        ),
        name="pack",
    )(*fixed(gate, up, down))


def merge_kernel(*refs):
    ins, outs, rows_ref = refs[:PLANE], refs[PLANE:-1], refs[-1]
    _, x, c, _ = place()
    group = ins[0].shape[1] // 3
    tall = 2 * group
    for k, out in enumerate(outs):
        for q in range(PLANE):
            xs, cs = jnp.bitwise_xor(x, q % X_COUNT), jnp.bitwise_xor(c, q // X_COUNT)
            slot = xs * CORE_COUNT + cs
            out[pl.ds(pl.multiple_of(slot * tall, tall), tall), :] = ins[q][k, :tall, :]
            rows_ref[pl.ds(pl.multiple_of(slot * group, group), group), :] = ins[q][
                k, tall:, :
            ].astype(F32)
        out[PLANE * tall :, :] = rows_ref[...].astype(BF16)


def merge(blocks):
    z_count, rows, part = blocks[0].shape
    return pl.pallas_call(
        merge_kernel,
        in_specs=[IN_VMEM] * PLANE,
        out_specs=[IN_VMEM] * z_count,
        out_shape=[jax.ShapeDtypeStruct((PLANE * rows, part), BF16)] * z_count,
        scratch_shapes=[pltpu.VMEM((PLANE * rows // 3, part), F32)],
        compiler_params=compiler_params(8),
        cost_estimate=pl.CostEstimate(
            flops=512 * z_count * rows * part, bytes_accessed=16 * rows * part, transcendentals=0
        ),
        name="merge",
    )(*blocks)


def load_kernel(mem, gif_in, uif_in, gw_in, uw_in, giu_ref, gw_ref, uw_ref, gif_ref, uif_ref, sem):
    copies = fetch(
        ((gif_in, gif_ref), (uif_in, uif_ref), (gw_in, gw_ref), (uw_in, uw_ref)), sem
    )
    for copy in copies[:2]:
        copy.wait()
    tall = 2 * mem * RANK
    for p in range(gif_ref.shape[0] // mem):
        rows = [ref[p * mem + m].astype(F32) for ref in (gif_ref, uif_ref) for m in range(mem)]
        giu_ref[p * tall : (p + 1) * tall] = jnp.concatenate(rows, axis=0).astype(BF16)
    for copy in copies[2:]:
        copy.wait()


def load(gif, uif, gw, uw, mem):
    members, rank, width = gif.shape
    return pl.pallas_call(
        functools.partial(load_kernel, mem),
        in_specs=[IN_HBM] * 4,
        out_specs=[IN_VMEM] * 3,
        out_shape=[
            pltpu.VMEM((2 * members * rank, width), BF16),
            pltpu.VMEM(gw.shape, BF16),
            pltpu.VMEM(uw.shape, BF16),
        ],
        scratch_shapes=[pltpu.VMEM(gif.shape, BF16)] * 2 + [pltpu.SemaphoreType.DMA((4,))],
        compiler_params=compiler_params(16),
        cost_estimate=pl.CostEstimate(
            flops=1024 * gw.size, bytes_accessed=4 * gw.size, transcendentals=0
        ),
        name="load",
    )(*fixed(gif, uif, gw, uw))


def scaled(ranks_ref, members, value, first, number):
    member = iota((value.shape[0], 1), 0) // RANK % number
    rank = jnp.zeros(member.shape, jnp.int32)
    for m in range(number):
        rank = jnp.where(member == m, ranks_ref[first + m], rank)
    return (value * (rank.astype(F32) / (members - 1) - 0.5)).astype(BF16)


def turn_into(out_ref, in_ref):
    columns = min(256, in_ref.shape[1])
    for j in range(in_ref.shape[1] // columns):
        at = slice(j * columns, (j + 1) * columns)
        out_ref[at] = in_ref[:, at].T.astype(BF16)


def turn_kernel(mem, ranks_ref, gif_in, uif_in, out_ref, gif_ref, uif_ref, rows_ref, sem):
    for copy in fetch(((gif_in, gif_ref), (uif_in, uif_ref)), sem):
        copy.wait()
    members = gif_ref.shape[0]
    tall = 2 * mem * RANK
    for p in range(members // mem):
        pieces = [ref[p * mem + m].astype(F32) for ref in (gif_ref, uif_ref) for m in range(mem)]
        value = scaled(ranks_ref, members, jnp.concatenate(pieces, axis=0), p * mem, mem)
        rows_ref[p * tall : (p + 1) * tall] = value.astype(F32)
    turn_into(out_ref, rows_ref)


def turn(ranks, gif, uif, mem):
    members, rank, width = gif.shape
    lanes = 2 * members * rank
    return pl.pallas_call(
        functools.partial(turn_kernel, mem),
        in_specs=[IN_SMEM] + [IN_HBM] * 2,
        out_specs=IN_VMEM,
        out_shape=jax.ShapeDtypeStruct((width, lanes), BF16),
        scratch_shapes=[pltpu.VMEM(gif.shape, BF16)] * 2
        + [pltpu.VMEM((lanes, width), F32), pltpu.SemaphoreType.DMA((2,))],
        compiler_params=compiler_params(12),
        cost_estimate=pl.CostEstimate(
            flops=4096 * gif.size, bytes_accessed=8 * gif.size, transcendentals=0
        ),
        name="turn",
    )(ranks, *fixed(gif, uif))


def arrange_kernel(z_count, ranks_ref, right_in, dw_in, *refs):
    gots = refs[:z_count]
    gu_ref, d_ref, dt_ref, right_ref, sright_ref, dw_ref = refs[z_count : z_count + 6]
    raw_ref, rows_ref, sem = refs[z_count + 6 :]
    copies = fetch(((right_in, raw_ref), (dw_in, dw_ref)), sem)
    z, _, _, _ = place()
    third = gots[0].shape[0] // 3
    members = raw_ref.shape[0]
    for k, got in enumerate(gots):
        zs = jnp.bitwise_xor(z, k)
        gu_ref[pl.ds(pl.multiple_of(zs * 2 * third, 2 * third), 2 * third), :] = got[: 2 * third, :]
        down_at = pl.ds(pl.multiple_of(zs * third, third), third)
        d_ref[down_at, :] = got[2 * third :, :]
        rows_ref[down_at, :] = got[2 * third :, :].astype(F32)
    turn_into(dt_ref, rows_ref)
    copies[0].wait()
    number = 4
    tall = number * RANK
    for p in range(members // number):
        value = jnp.concatenate([raw_ref[p * number + m].astype(F32) for m in range(number)], axis=0)
        right_ref[p * tall : (p + 1) * tall] = value.astype(BF16)
        sright_ref[p * tall : (p + 1) * tall] = scaled(ranks_ref, members, value, p * number, number)
    copies[1].wait()


def arrange(ranks, gots, right, dw):
    hidden = gots[0].shape[1]
    members, rank, width = right.shape
    lanes = members * rank
    return pl.pallas_call(
        functools.partial(arrange_kernel, len(gots)),
        in_specs=[IN_SMEM] + [IN_HBM] * 2 + [IN_VMEM] * len(gots),
        out_specs=[IN_VMEM] * 6,
        out_shape=[
            pltpu.VMEM((2 * lanes, hidden), BF16),
            pltpu.VMEM((lanes, hidden), BF16),
            pltpu.VMEM((hidden, lanes), BF16),
            pltpu.VMEM((lanes, width), BF16),
            pltpu.VMEM((lanes, width), BF16),
            pltpu.VMEM(dw.shape, BF16),
        ],
        scratch_shapes=[
            pltpu.VMEM(right.shape, BF16),
            pltpu.VMEM((lanes, hidden), F32),
            pltpu.SemaphoreType.DMA((2,)),
        ],
        compiler_params=compiler_params(16),
        cost_estimate=pl.CostEstimate(
            flops=1024 * dw.size, bytes_accessed=4 * dw.size, transcendentals=0
        ),
        name="arrange",
    )(ranks, *fixed(right, dw), *gots)


def unit_members(units, per_block, shifts, z, start):
    members = []
    for w in range(units):
        unit = start(w)
        zs = jnp.int32(0)
        for b, shift in enumerate(shifts):
            zs = jnp.where(unit // per_block == b, jnp.bitwise_xor(z, shift), zs)
        members.append(zs * per_block + unit % per_block)
    return members


def lane_members(shape, group):
    lane = iota(shape, 1)
    return lane // (2 * group) * (group // RANK) + lane % group // RANK


def gate_up_kernel(shifts, hid_count, mem_local, *refs):
    blocks = len(shifts)
    pieces = refs[: PLANE * blocks]
    gw_ref, uw_ref, giu_ref = refs[PLANE * blocks : PLANE * blocks + 3]
    sends = refs[PLANE * blocks + 3 : PLANE * blocks + 2 + hid_count]
    keep_ref, keep_proj_ref, rows_ref = refs[PLANE * blocks + 2 + hid_count :]
    z, x, c, y = place()
    per_block = PLANE * mem_local
    units = per_block * blocks
    per_part = units // hid_count
    part_rows = per_part * SAMPLE_LENGTH
    hidden = keep_ref.shape[1] // 2
    columns = min(256, hidden)
    group = mem_local * RANK
    for b in range(blocks):
        for q in range(PLANE):
            rx, rc = q % 2, q // 2
            piece = pieces[b * PLANE + q]
            slot = b * PLANE + jnp.bitwise_xor(x, rx) * CORE_COUNT + jnp.bitwise_xor(c, rc)
            for m in range(mem_local):
                unit = slot * mem_local + m
                rel = lax.rem(unit // per_part - y - 1 + hid_count, hid_count)
                row = (rel * per_part + unit % per_part) * SAMPLE_LENGTH
                rows_ref[pl.ds(pl.multiple_of(row, SAMPLE_LENGTH), SAMPLE_LENGTH), :] = piece[
                    m * SAMPLE_LENGTH : (m + 1) * SAMPLE_LENGTH, :
                ]
    members = unit_members(
        units,
        per_block,
        shifts,
        z,
        lambda p: lax.rem(p // per_part + y + 1, hid_count) * per_part + p % per_part,
    )
    rows = rows_ref[...]
    projected = dot_nt(rows, giu_ref[...])
    mine = row_members(projected.shape, members) == lane_members(projected.shape, group)
    high, low = split_high_low(jnp.where(mine, projected, 0.0))
    shape = (projected.shape[1], LANES)
    lane = iota(shape, 0) % RANK + 2 * RANK * (iota(shape, 0) // group % 2)

    def pick(level):
        return (lane + RANK * level == iota(shape, 1)).astype(F32).astype(BF16)

    packed = (dot(high, pick(0)) + dot(low, pick(1))).astype(BF16)
    for s in range(hid_count - 1):
        sends[s][:, 2 * hidden :] = packed[s * part_rows : (s + 1) * part_rows]
    keep_proj_ref[...] = packed[(hid_count - 1) * part_rows :]
    for j in range(hidden // columns):
        for index, ref in enumerate((gw_ref, uw_ref)):
            value = dot(rows, ref[:, j * columns : (j + 1) * columns])
            at = slice(index * hidden + j * columns, index * hidden + (j + 1) * columns)
            for s in range(hid_count - 1):
                sends[s][:, at] = value[s * part_rows : (s + 1) * part_rows].astype(BF16)
            keep_ref[:, at] = value[(hid_count - 1) * part_rows :]


def gate_up(pieces, gw, uw, giu, shifts, hid_count):
    rows, width = pieces[0].shape
    hidden = gw.shape[1]
    total = rows * PLANE * len(shifts)
    part = total // hid_count
    send_shape = (part, 2 * hidden + LANES)
    return pl.pallas_call(
        functools.partial(gate_up_kernel, shifts, hid_count, rows // SAMPLE_LENGTH),
        in_specs=[IN_VMEM] * (len(pieces) + 3),
        out_specs=[IN_VMEM] * (hid_count + 1),
        out_shape=[jax.ShapeDtypeStruct(send_shape, BF16)] * (hid_count - 1)
        + [
            jax.ShapeDtypeStruct((part, 2 * hidden), F32),
            jax.ShapeDtypeStruct((part, LANES), BF16),
        ],
        scratch_shapes=[pltpu.VMEM((total, width), BF16)],
        compiler_params=compiler_params(24),
        cost_estimate=pl.CostEstimate(
            flops=4 * total * width * hidden, bytes_accessed=4 * width * hidden, transcendentals=0
        ),
        name="gate_up",
    )(*pieces, gw, uw, giu)


def hidden_kernel(shifts, hid_count, mem_local, scale, *refs):
    keep_ref, keep_proj = refs[:2]
    recvs = refs[2 : 1 + hid_count]
    cols_ref, out_ref = refs[1 + hid_count :]
    z, _, _, y = place()
    per_block = PLANE * mem_local
    per_part = per_block * len(shifts) // hid_count
    lanes, hidden = cols_ref.shape
    group = mem_local * RANK
    rows = keep_proj.shape[0]
    members = unit_members(per_part, per_block, shifts, z, lambda w: y * per_part + w)
    mine = row_members((rows, lanes), members) == lane_members((rows, lanes), group)
    source, target = iota((LANES, lanes), 0), iota((LANES, lanes), 1)
    base = target % RANK + 2 * RANK * (target // group % 2)
    spread = ((source == base) | (source == base + RANK)).astype(F32).astype(BF16)
    value = dot(keep_proj[...], spread)
    for ref in recvs:
        value = value + dot(ref[:, 2 * hidden :], spread)
    value = jnp.where(mine, value, 0.0) * scale
    of_gate = iota((rows, lanes), 1) // group % 2 == 0
    gate_high, gate_low = split_high_low(jnp.where(of_gate, value, 0.0))
    up_high, up_low = split_high_low(jnp.where(of_gate, 0.0, value))
    stack = jnp.concatenate([gate_high, gate_low, up_high, up_low], axis=0)
    columns = min(256, hidden)
    for j in range(hidden // columns):
        lowrank = dot(stack, cols_ref[:, j * columns : (j + 1) * columns])

        def total(index):
            at = slice(index * hidden + j * columns, index * hidden + (j + 1) * columns)
            value = keep_ref[:, at]
            for ref in recvs:
                value = value + ref[:, at].astype(F32)
            first = 2 * index * rows
            return value + (lowrank[first : first + rows] + lowrank[first + rows : first + 2 * rows])

        gate, up = total(0), total(1)
        out_ref[:, j * columns : (j + 1) * columns] = (
            gate / (1.0 + jnp.exp(-gate)) * up
        ).astype(BF16)


def make_hidden(keep, keep_proj, recvs, cols, shifts, hid_count, mem_local, scale):
    part = keep.shape[0]
    hidden = keep.shape[1] // 2
    lanes = cols.shape[0]
    return pl.pallas_call(
        functools.partial(hidden_kernel, shifts, hid_count, mem_local, scale),
        in_specs=[IN_VMEM] * (3 + len(recvs)),
        out_specs=IN_VMEM,
        out_shape=jax.ShapeDtypeStruct((part, hidden), BF16),
        compiler_params=compiler_params(12),
        cost_estimate=pl.CostEstimate(
            flops=8 * part * lanes * hidden, bytes_accessed=8 * part * hidden, transcendentals=0
        ),
        name="make_hidden",
    )(keep, keep_proj, *recvs, cols)


def down_kernel(shifts, hid_count, mem_local, scale, *refs):
    blocks = len(shifts)
    parts = refs[:hid_count]
    dw_ref, cols_ref, right_ref, send_ref, keep_ref, rows_ref = refs[hid_count:]
    z, x, c, y = place()
    units = PLANE * mem_local * blocks
    per_part = units // hid_count
    half, width = send_ref.shape
    for s in range(hid_count):
        for w in range(per_part):
            unit = lax.rem(y + s, hid_count) * per_part + w
            b = unit // (PLANE * mem_local)
            rx = jnp.bitwise_xor(unit // (CORE_COUNT * mem_local) % X_COUNT, x)
            rc = jnp.bitwise_xor(unit // mem_local % CORE_COUNT, c)
            slot = ((1 - rc) * X_COUNT + 1 - rx) * blocks + b
            row = (slot * mem_local + unit % mem_local) * SAMPLE_LENGTH
            rows_ref[pl.ds(pl.multiple_of(row, SAMPLE_LENGTH), SAMPLE_LENGTH), :] = parts[s][
                w * SAMPLE_LENGTH : (w + 1) * SAMPLE_LENGTH, :
            ]
    members = []
    for p in range(units):
        slot, m = p // mem_local, p % mem_local
        q, b = slot // blocks, slot % blocks
        xs = jnp.bitwise_xor(x, 1 - q % X_COUNT)
        cs = jnp.bitwise_xor(c, 1 - q // X_COUNT)
        zs = jnp.bitwise_xor(z, shifts[b])
        members.append(((zs * X_COUNT + xs) * CORE_COUNT + cs) * mem_local + m)
    rows = rows_ref[...]
    projected = dot_nt(rows, cols_ref[...])
    mine = row_members(projected.shape, members) == iota(projected.shape, 1) // RANK
    both = jnp.concatenate(split_high_low(jnp.where(mine, projected, 0.0) * scale), axis=1)
    columns = min(256, width)
    for j in range(width // columns):
        at = slice(j * columns, (j + 1) * columns)
        right = right_ref[:, at]
        value = dot(rows, dw_ref[:, at]) + dot(both, jnp.concatenate([right, right], axis=0))
        send_ref[:, at] = value[:half].astype(BF16)
        keep_ref[:, at] = value[half:]


def down(parts, dw, cols, right, shifts, hid_count, mem_local, scale):
    part, hidden = parts[0].shape
    width = dw.shape[1]
    total = part * hid_count
    return pl.pallas_call(
        functools.partial(down_kernel, shifts, hid_count, mem_local, scale),
        in_specs=[IN_VMEM] * (hid_count + 3),
        out_specs=[IN_VMEM] * 2,
        out_shape=[
            jax.ShapeDtypeStruct((total // 2, width), BF16),
            jax.ShapeDtypeStruct((total // 2, width), F32),
        ],
        scratch_shapes=[pltpu.VMEM((total, hidden), BF16)],
        compiler_params=compiler_params(16),
        cost_estimate=pl.CostEstimate(
            flops=2 * total * width * hidden, bytes_accessed=2 * width * hidden, transcendentals=0
        ),
        name="down",
    )(*parts, dw, cols, right)


def input_step_kernel(index, group, factor, in_ref, cols_ref, out_ref):
    rows = out_ref.shape[0]
    left = in_ref[pl.ds(pl.multiple_of(pl.program_id(0) * rows, LANES), rows), :]
    belongs = iota(left.shape, 1) // group % 2 == index
    left = jnp.where(belongs, left.astype(F32), 0.0).astype(BF16)
    out_ref[...] = factor * dot(left, cols_ref[...])


def input_step(index, group, factor, in_factor, cols):
    width, lanes = in_factor.shape
    hidden = cols.shape[1]
    rows = min(512, width)
    return pl.pallas_call(
        functools.partial(input_step_kernel, index, group, factor),
        grid=(width // rows,),
        in_specs=[IN_VMEM] * 2,
        out_specs=pl.BlockSpec((rows, hidden), lambda i: (i, 0)),
        out_shape=jax.ShapeDtypeStruct((width, hidden), F32),
        compiler_params=compiler_params(12),
        cost_estimate=pl.CostEstimate(
            flops=8 * width * lanes * hidden, bytes_accessed=4 * width * hidden, transcendentals=0
        ),
    )(in_factor, cols)


def down_step_kernel(factor, left_ref, right_ref, out_ref):
    rows = out_ref.shape[0]
    left = left_ref[pl.ds(pl.multiple_of(pl.program_id(0) * rows, LANES), rows), :]
    out_ref[...] = factor * dot(left, right_ref[...])


def down_step(factor, left, right):
    hidden, lanes = left.shape
    width = right.shape[1]
    rows = min(256, hidden)
    return pl.pallas_call(
        functools.partial(down_step_kernel, factor),
        grid=(hidden // rows,),
        in_specs=[IN_VMEM] * 2,
        out_specs=pl.BlockSpec((rows, width), lambda i: (i, 0)),
        out_shape=jax.ShapeDtypeStruct((hidden, width), F32),
        compiler_params=compiler_params(12),
        cost_estimate=pl.CostEstimate(
            flops=8 * width * lanes * hidden, bytes_accessed=4 * width * hidden, transcendentals=0
        ),
        name="down_step",
    )(left, right)


def local(
    tokens,
    fitness_ranks,
    gate_weight,
    up_weight,
    down_weight,
    gate_input_factor,
    up_input_factor,
    down_right,
    gate_output_factor,
    up_output_factor,
    down_left,
):
    pop_count = lax.axis_size("pop")
    hid_count = lax.axis_size("hid")
    z_count = pop_count // PLANE
    assert z_count & (z_count - 1) == 0
    tok_local, _ = tokens.shape
    mem_local = tok_local // SAMPLE_LENGTH
    members = mem_local * pop_count
    scale_in = 0.5 / math.sqrt(MODEL_WIDTH * RANK)
    scale_out = 0.5 / math.sqrt(HIDDEN_UNITS * RANK)
    factor = 1.0 / math.sqrt(members * RANK)

    everyone = range(pop_count)
    core_pairs = [(i, i ^ 1) for i in everyone]
    x_pairs = [(i, i ^ CORE_COUNT) for i in everyone]

    def forward(k):
        return [(i, i ^ (k * PLANE)) for i in everyone]

    def along(v, pairs):
        return lax.ppermute(v, "pop", pairs)

    groups = GROUPS(z_count)

    blocks = {}
    for k in range(z_count):
        own = tokens if k == 0 else along(tokens, forward(k))
        from_x = along(own, x_pairs)
        from_core = along(own, core_pairs)
        from_both = along(from_x, core_pairs)
        blocks[k] = [own, from_x, from_core, from_both]

    near, near_x, far, far_x = pack(gate_output_factor, up_output_factor, down_left, z_count)
    from_x = along(near_x, x_pairs)
    far_x = along(far_x, core_pairs)
    far = along(far, core_pairs)
    far_x = along(far_x, x_pairs)
    joined = merge([near, from_x, far, far_x])
    gots = []
    for k in range(z_count):
        gots.append(along(joined[k], forward(k)) if k else joined[k])
    giu, gate_v, up_v = load(gate_input_factor, up_input_factor, gate_weight, up_weight, mem_local)
    scaled_giu = turn(fitness_ranks, gate_input_factor, up_input_factor, mem_local)
    gu_cols, d_cols, d_turned, right, scaled_right, down_v = arrange(
        fitness_ranks, gots, down_right, down_weight
    )

    total = None
    for shifts in groups:
        pieces = [piece for k in shifts for piece in blocks[k]]
        *sends, keep, keep_proj = gate_up(pieces, gate_v, up_v, giu, shifts, hid_count)
        recvs = [
            lax.ppermute(v, "hid", [(i, (i + s + 1) % hid_count) for i in range(hid_count)])
            for s, v in enumerate(sends)
        ]
        mine = make_hidden(keep, keep_proj, recvs, gu_cols, shifts, hid_count, mem_local, scale_in)
        parts = [mine] + [
            lax.ppermute(mine, "hid", [((i + s) % hid_count, i) for i in range(hid_count)])
            for s in range(1, hid_count)
        ]
        send, held = down(parts, down_v, d_cols, right, shifts, hid_count, mem_local, scale_out)
        held = held + along(send, core_pairs).astype(F32)
        half = held.shape[0] // 2
        held = held[half:] + along(held[:half].astype(BF16), x_pairs).astype(F32)
        for b, k in enumerate(shifts):
            piece = held[b * tok_local : (b + 1) * tok_local]
            if k:
                piece = along(piece.astype(BF16), forward(k)).astype(F32)
            total = piece if total is None else total + piece
    mixed = total.astype(BF16)

    group = mem_local * RANK
    gate_step = input_step(0, group, factor, scaled_giu, gu_cols)
    up_step = input_step(1, group, factor, scaled_giu, gu_cols)
    step = down_step(factor, d_turned, scaled_right)
    return (mixed, gate_step, up_step, step)


def GROUPS(z_count):
    return [(1,), (0,), *[tuple(range(z_count))[i : i + 2] for i in range(2, z_count, 2)]]


def solution(mesh):
    in_specs = (
        P("pop", "hid"),
        P(),
        P("hid", "pop"),
        P("hid", "pop"),
        P("pop", "hid"),
        P(None, None, "hid"),
        P(None, None, "hid"),
        P(None, None, "hid"),
        P("pop", None, None),
        P("pop", None, None),
        P("pop", None, None),
    )
    out_specs = (P("pop", "hid"), P("hid", "pop"), P("hid", "pop"), P("pop", "hid"))
    return jax.shard_map(local, mesh=mesh, in_specs=in_specs, out_specs=out_specs, check_vma=False)
```
